32 devices in a mesh: dp: 8 (over y, x, core), tp: 4 (over z).
Axes of the slice: x: 2, y: 2, z: 4, core: 2. Of those that a mesh axis runs over, the one named last changes fastest.
Arguments:
- inputs: bfloat16 [8, 768, 1280], P('dp', 'tp'), may hold values from -6 to 6
- saved_hidden: bfloat16 [8, 768, 5120], P('dp', None, 'tp'), may hold values from -8 to 8
- upstream: bfloat16 [8, 768, 1280], P('dp', 'tp'), may hold values from -6 to 6
- w_in: bfloat16 [1280, 5120], P(None, 'tp'), may hold values from -0.15625 to 0.15625
- w_out: bfloat16 [5120, 1280], P('tp'), may hold values from -0.078125 to 0.078125
- kernel: float32 [7, 1280], replicated, may hold values from -2 to 2
Outputs:
- grad_inputs: bfloat16 [8, 768, 1280], P('dp', 'tp')
- grad_w_in: float32 [1280, 5120], P(None, 'tp')
- grad_w_out: float32 [5120, 1280], P('tp')
- grad_bias: float32 [5120], P('tp')
- grad_kernel: float32 [7, 1280], replicated
The draws below stay inside these ranges and needn't reach their ends.
All inputs are finite; a program needn't handle non-finite values.
Results may differ from the reference program's by a relative error of at most 0.02.
Values may be sent and summed in bfloat16 or wider, within the bound.
A program may use at most 128 MiB of HBM per device.

```python
from functools import partial
import jax
import jax.numpy as jnp
from jax import lax

D = 1280
FF = 5120
KW = 7
SEQ = 768
SEQS = 8
N_TP = 4


def shard_levels(stream_key, dims, pieces, low, top_value):
    gain = 1.0
    for position, blocks in pieces:
        draws = jax.random.uniform(jax.random.fold_in(jax.random.fold_in(stream_key, 6), position), (blocks,), jnp.float32, low / len(pieces), top_value / len(pieces))
        gain = gain * jnp.repeat(jnp.exp(draws), dims[position] // blocks).reshape((-1,) + (1,) * (len(dims) - 1 - position))
    return gain


def normal_values(rng, dims, width, reach, split=(), dtype=jnp.bfloat16):
    values = width * jax.random.normal(rng, dims, jnp.float32)
    if split:
        values = values * shard_levels(rng, dims, split, -0.22, 0.18)
    return jnp.clip(values, -reach, reach).astype(dtype)


def setup_inputs(seed: int = 0) -> dict:
    key_of = jax.random.split(jax.random.key(seed), 7)
    return {
        "inputs": normal_values(key_of[0], (SEQS, SEQ, D), 1.0, 6.0, ((0, 8), (1, 4))),
        "saved_hidden": normal_values(key_of[1], (SEQS, SEQ, FF), 1.5, 8.0, ((0, 8), (2, 4))),
        "upstream": normal_values(key_of[2], (SEQS, SEQ, D), 1.0, 6.0, ((0, 8), (1, 4))),
        "w_in": normal_values(key_of[3], (D, FF), D ** -0.5, 0.15625, ((1, 4),)),
        "w_out": normal_values(key_of[4], (FF, D), FF ** -0.5, 0.078125, ((0, 4),)),
        "kernel": normal_values(key_of[5], (KW, D), 0.3, 2.0, (), jnp.float32),
    }


def gelu_exact(value):
    return jax.nn.gelu(value, approximate=False)

def one_sequence(carry, items, w_in, w_out, kernel):
    total_in, total_out, total_bias, total_kernel = carry
    inputs, hidden, upstream = items
    length = inputs.shape[0]
    inputs_f = inputs.astype(jnp.float32)
    padded = jnp.pad(inputs_f, ((3, 3), (0, 0)))
    mixed = inputs_f
    for tap in range(KW):
        mixed = mixed + kernel[tap] * padded[tap:tap + length]
    mixed = mixed.astype(jnp.bfloat16)
    hidden_f = hidden.astype(jnp.float32)
    activated = gelu_exact(hidden_f).astype(jnp.bfloat16)
    back_hidden = jnp.dot(upstream, w_out.T, preferred_element_type=jnp.float32)
    grad_hidden = jax.vjp(gelu_exact, hidden_f)[1](back_hidden)[0].astype(jnp.bfloat16)
    total_out = total_out + jnp.dot(activated.T, upstream, preferred_element_type=jnp.float32)
    total_in = total_in + jnp.dot(mixed.T, grad_hidden, preferred_element_type=jnp.float32)
    total_bias = total_bias + lax.optimization_barrier(jnp.sum(grad_hidden.astype(jnp.float32), axis=0))
    block = FF // N_TP
    hidden_blocks = grad_hidden.reshape(length, N_TP, block).astype(jnp.float32)
    weight_blocks = w_in.reshape(D, N_TP, block).astype(jnp.float32)
    parts = jnp.einsum('lnf,dnf->nld', hidden_blocks, weight_blocks).astype(jnp.bfloat16)
    parts = lax.optimization_barrier(parts).astype(jnp.float32)
    grad_mixed = (upstream.astype(jnp.float32) + lax.optimization_barrier(jnp.sum(parts, axis=0))).astype(jnp.bfloat16)
    grad_f = grad_mixed.astype(jnp.float32)
    grad_pad = jnp.pad(grad_f, ((3, 3), (0, 0)))
    grad_inputs = grad_f
    taps = []
    for tap in range(KW):
        grad_inputs = grad_inputs + kernel[tap] * grad_pad[6 - tap:6 - tap + length]
        taps.append(lax.optimization_barrier(jnp.sum(grad_f * padded[tap:tap + length], axis=0)))
    total_kernel = total_kernel + jnp.stack(taps)
    return ((total_in, total_out, total_bias, total_kernel), grad_inputs.astype(jnp.bfloat16))

def reference(inputs, saved_hidden, upstream, w_in, w_out, kernel):
    start = (jnp.zeros((D, FF), jnp.float32), jnp.zeros((FF, D), jnp.float32), jnp.zeros((FF,), jnp.float32), jnp.zeros((KW, D), jnp.float32))
    step = partial(one_sequence, w_in=w_in, w_out=w_out, kernel=kernel)
    totals, grad_inputs = lax.scan(step, start, (inputs, saved_hidden, upstream))
    return (grad_inputs, totals[0], totals[1], totals[2], totals[3])
```

```python
import functools

import jax
import jax.numpy as jnp
from jax import lax
from jax.experimental import pallas as pl
from jax.experimental.pallas import tpu as pltpu
from jax.sharding import PartitionSpec as P

KW = 7
EDGE = 16
F32 = jnp.float32
BF16 = jnp.bfloat16
MESH = pl.DeviceIdType.MESH


def dot(a, b, dims):
    return lax.dot_general(a, b, (dims, ((), ())), preferred_element_type=F32)


def chunk_of(size):
    return 256 if size % 256 == 0 else size


def body(
    n, dp_size, rows_in, rows_out,
    x_ref, h_ref, up_ref, win_ref, wout_ref, k_ref,
    gin_ref, gwin_ref, gwout_ref, small_ref,
    act, gh, up_all, mix_all, part, zrecv, xpad, gpad, acc_in, acc_out, bias,
    psend_in, psend_out, precv_in, precv_out, rsend_in, rsend_out, rrecv_in, rrecv_out,
    k1, k2,
    hs, hr, us, ur, ms, mr, zs, zr, ps, pr, rs, rr, ds, dr, gs, gr, k1s, k1r, k2s, k2r,
):
    chips = dp_size // 2
    me = lax.axis_index("tp")
    dp = lax.axis_index("dp")
    core = lax.rem(dp, 2)
    chip = dp // 2
    tokens, width = x_ref.shape
    hidden = h_ref.shape[2]
    wide = chunk_of(width)
    tall = chunk_of(hidden)

    def flip(i):
        return jnp.where(i < chips // 2, i, chips // 2 + chips - 1 - i)

    pos = flip(chip)
    spots = (pos, lax.rem(chips - pos, chips))
    after = (
        flip(lax.rem(pos + 1, chips)) * 2 + core,
        flip(lax.rem(pos + chips - 1, chips)) * 2 + core,
    )
    partner = dp + 1 - 2 * core

    barrier = pltpu.get_barrier_semaphore()
    for j in range(1, n):
        pl.semaphore_signal(
            barrier, inc=1, device_id=(dp, lax.rem(me + j, n)), device_id_type=MESH
        )
    for j in range(1, dp_size):
        pl.semaphore_signal(
            barrier, inc=1, device_id=(lax.rem(dp + j, dp_size), me), device_id_type=MESH
        )
    pl.semaphore_wait(barrier, n - 1 + dp_size - 1)

    def send(src, dst, s, r, to):
        return pltpu.make_async_remote_copy(
            src_ref=src, dst_ref=dst, send_sem=s, recv_sem=r, device_id=to, device_id_type=MESH
        )

    pending = []

    def start(cond, make):
        if cond is None:
            make().start()
        else:

            @pl.when(cond)
            def _():
                make().start()

        pending.append((cond, make))

    ways = (0, 1)
    step_of = (1, -1)
    room = (me, n - 1 - me)
    ahead = (n - 1 - me, me)

    def chain(buf, s, r, d, back):
        block = me - step_of[d] * back
        safe = jnp.clip(block, 0, n - 1)
        to = (dp, jnp.clip(me + step_of[d], 0, n - 1))
        return send(buf.at[safe], buf.at[safe], s.at[d, safe], r.at[d, safe], to)

    def edge(src, low, high, s, r, d):
        to = (dp, jnp.clip(me + step_of[d], 0, n - 1))
        if d == 0:
            return send(
                src.at[pl.ds(high, EDGE)], low, s.at[d], r.at[d], to
            )
        return send(src.at[pl.ds(0, EDGE)], low, s.at[d], r.at[d], to)

    def x_edge(d):
        if d == 0:
            return edge(x_ref, xpad.at[pl.ds(0, EDGE)], tokens - EDGE, hs, hr, 0)
        return edge(x_ref, xpad.at[pl.ds(EDGE + tokens, EDGE)], 0, hs, hr, 1)

    def up_first(d):
        to = (dp, jnp.clip(me + step_of[d], 0, n - 1))
        return send(up_ref, up_all.at[me], us.at[d, me], ur.at[d, me], to)

    for d in ways:
        start(ahead[d] > 0, functools.partial(x_edge, d))
    for d in ways:
        start(ahead[d] > 0, functools.partial(up_first, d))

    if act.shape[2] > hidden:
        act[...] = jnp.zeros_like(act)

    def gelu_step(i, _):
        b = i // (tokens // 32)
        at = pl.ds(pl.multiple_of(lax.rem(i, tokens // 32) * 32, 32), 32)
        v = h_ref[b, at, :].astype(F32)
        cdf = 0.5 + 0.5 * lax.erf(v * 0.7071067811865476)
        act[b, at, pl.ds(0, hidden)] = (v * cdf).astype(BF16)
        gh[b, at, :] = (cdf + v * (0.3989422804014327 * jnp.exp(-0.5 * v * v))).astype(BF16)
        return 0

    lax.fori_loop(0, n * (tokens // 32), gelu_step, 0)
    xpad[pl.ds(EDGE, tokens), :] = x_ref[...]

    @pl.when(me == 0)
    def _():
        xpad[pl.ds(0, EDGE), :] = jnp.zeros((EDGE, width), BF16)
        gpad[pl.ds(0, EDGE), :] = jnp.zeros((EDGE, width), BF16)

    @pl.when(me == n - 1)
    def _():
        xpad[pl.ds(EDGE + tokens, EDGE), :] = jnp.zeros((EDGE, width), BF16)
        gpad[pl.ds(EDGE + tokens, EDGE), :] = jnp.zeros((EDGE, width), BF16)

    for d in ways:

        @pl.when(room[d] > 0)
        def _(d=d):
            x_edge(d).wait_recv()

    def mix_step(i, _):
        at = pl.ds(pl.multiple_of(i * 128, 128), 128)
        x = xpad[:, at].astype(F32)
        taps = k_ref[:, at]
        total = x[EDGE : EDGE + tokens]
        for tap in range(KW):
            low = EDGE - 3 + tap
            total = total + taps[tap : tap + 1] * x[low : low + tokens]
        mix_all[me, :, at] = total.astype(BF16)
        return 0

    lax.fori_loop(0, width // 128, mix_step, 0)

    bias[...] = jnp.zeros_like(bias)
    acc_in[...] = jnp.zeros_like(acc_in)
    acc_out[...] = jnp.zeros_like(acc_out)

    def use_upstream(src, b):
        def back_step(i, _):
            at = pl.ds(pl.multiple_of(i * tall, tall), tall) if tall < hidden else pl.ds(0, hidden)
            back = dot(src[...], wout_ref[at, :], ((1,), (1,)))
            grad = (gh[b, :, at].astype(F32) * back).astype(BF16)
            gh[b, :, at] = grad
            bias[:, at] += jnp.sum(grad.astype(F32), axis=0, keepdims=True)
            return 0

        lax.fori_loop(0, hidden // tall, back_step, 0)

        def out_step(i, _):
            at = pl.ds(pl.multiple_of(i * wide, wide), wide)
            acc_out[:, at] += dot(act[b], src[:, at], ((0,), (0,)))
            part[b, :, at] = dot(gh[b], win_ref[at, :], ((1,), (1,))).astype(BF16)
            return 0

        lax.fori_loop(0, width // wide, out_step, 0)

    def use_mixed(b):
        def in_step(i, _):
            at = pl.ds(pl.multiple_of(i * wide, wide), wide)
            acc_in[at, :] += dot(mix_all[b, :, at], gh[b], ((0,), (0,)))
            return 0

        lax.fori_loop(0, width // wide, in_step, 0)

    def mix_chain(d, back):
        return chain(mix_all, ms, mr, d, back)

    def up_chain(d, back):
        return chain(up_all, us, ur, d, back)

    for d in ways:
        start((ahead[d] > 0) & (room[d] == 0), functools.partial(mix_chain, d, 0))
    use_upstream(up_ref, me)
    for back in range(1, n):
        for d in ways:

            @pl.when(room[d] >= back)
            def _(d=d):
                up_chain(d, back).wait_recv()

            start((room[d] >= back) & (ahead[d] > 0), functools.partial(up_chain, d, back))
            start((room[d] == back) & (ahead[d] > 0), functools.partial(mix_chain, d, 0))
        for d in ways:

            @pl.when(room[d] >= back)
            def _(d=d):
                b = jnp.clip(me - step_of[d] * back, 0, n - 1)
                use_upstream(up_all.at[b], b)

    sets = (
        (acc_out, psend_out, precv_out, rsend_out, rrecv_out, gwout_ref, rows_out),
        (acc_in, psend_in, precv_in, rsend_in, rrecv_in, gwin_ref, rows_in),
    )

    def rows_at(w, half, d, block):
        rows = sets[w][6]
        return pl.ds(pl.multiple_of(((half * 2 + d) * chips + block) * rows, 8), rows)

    def pair_copy(w):
        return send(sets[w][1], sets[w][2], ps.at[w], pr.at[w], (partner, me))

    def pair_start(w):
        for d in ways:
            for block in range(chips):
                sets[w][1][d, block] = sets[w][0][rows_at(w, 1 - core, d, block), :].astype(BF16)
        start(None, functools.partial(pair_copy, w))

    def own(w, d, block):
        return sets[w][0][rows_at(w, core, d, block), :] + sets[w][2][d, block].astype(F32)

    def ring_reduce(w, d, s):
        return send(
            sets[w][3].at[d, s], sets[w][4].at[d, s], rs.at[w, d, s], rr.at[w, d, s], (after[d], me)
        )

    def ring_gather(w, d, s):
        block = lax.rem(spots[d] + 1 - s + chips, chips)
        ref = sets[w][5].at[core, d, block]
        at = chips - 1 + s
        return send(ref, ref, rs.at[w, d, at], rr.at[w, d, at], (after[d], me))

    def across(w, d, block, half):
        ref = sets[w][5].at[half, d, block]
        return send(ref, ref, ds.at[w, d, block], dr.at[w, d, block], (partner, me))

    last = 2 * (chips - 1)

    def ring_step(w, s):
        if s > last:
            return
        if s == 0:
            pair_copy(w).wait_recv()
        for d in ways:
            spot = spots[d]
            if s < chips:
                block = lax.rem(spot - s + chips, chips)
                value = own(w, d, block)
                if s > 0:
                    ring_reduce(w, d, s - 1).wait_recv()
                    value = value + sets[w][4][d, s - 1].astype(F32)
                if s < chips - 1:
                    sets[w][3][d, s] = value.astype(BF16)
                    start(None, functools.partial(ring_reduce, w, d, s))
                    continue
                sets[w][5][core, d, block] = value.astype(BF16)
            else:
                block = lax.rem(spot + 1 - (s - chips + 1) + chips, chips)
                ring_arrive(w, d, s - chips).wait_recv()
            if s < last:
                start(None, functools.partial(ring_gather, w, d, s - chips + 1))
            start(None, functools.partial(across, w, d, block, core))

    def ring_arrive(w, d, s):
        block = lax.rem(spots[d] - s + chips, chips)
        ref = sets[w][5].at[core, d, block]
        at = chips - 1 + s
        return send(ref, ref, rs.at[w, d, at], rr.at[w, d, at], (after[d], me))

    def ring_end(w):
        for d in ways:
            for block in range(chips):
                across(w, d, block, 1 - core).wait_recv()

    def target(d, t, behind):
        place = room[d] - behind
        block = n - 1 - t + place
        return block if d == 0 else n - 1 - block

    def z_slot(d, block, owner):
        return jnp.where((block == owner) & (d == 1), n, block)

    def z_send(d, t):
        block = jnp.clip(target(d, t, 0), 0, n - 1)
        to = jnp.clip(me + step_of[d], 0, n - 1)
        return send(
            part.at[block], zrecv.at[z_slot(d, block, to)], zs.at[d, t], zr.at[d, t], (dp, to)
        )

    def z_arrive(d, t):
        block = jnp.clip(target(d, t, 1), 0, n - 1)
        slot = zrecv.at[z_slot(d, block, me)]
        return send(slot, slot, zs.at[d, t], zr.at[d, t], (dp, jnp.clip(me + 1, 0, n - 1)))

    def z_step(t):
        if t > n - 1:
            return
        for d in ways:
            if t > 0:

                @pl.when((room[d] >= 1) & (room[d] - 1 <= t - 1))
                def _(d=d):
                    z_arrive(d, t - 1).wait_recv()
                    if t < n - 1:
                        block = jnp.clip(target(d, t - 1, 1), 0, n - 1)
                        part[block] = (
                            part[block].astype(F32) + zrecv[z_slot(d, block, me)].astype(F32)
                        ).astype(BF16)

            if t < n - 1:
                start((room[d] <= t) & (ahead[d] > 0), functools.partial(z_send, d, t))

    pair_start(0)
    z_step(0)
    use_mixed(me)
    ring_step(0, 0)
    per = -(-last // (n - 1))
    done = 1
    for back in range(1, n):
        for d in ways:

            @pl.when(room[d] >= back)
            def _(d=d):
                mix_chain(d, back).wait_recv()

            start((room[d] >= back) & (ahead[d] > 0), functools.partial(mix_chain, d, back))
        for d in ways:

            @pl.when(room[d] >= back)
            def _(d=d):
                use_mixed(jnp.clip(me - step_of[d] * back, 0, n - 1))

        if back < n - 1:
            z_step(back)
        for _ in range(per):
            if back < n - 1:
                ring_step(0, done)
                done += 1
    pair_start(1)
    while done <= last:
        ring_step(0, done)
        done += 1
    ring_step(1, 0)
    z_step(n - 1)

    def sum_step(i, _):
        at = pl.ds(pl.multiple_of(i * 128, 128), 128)
        total = part[me, :, at].astype(F32)
        left = jnp.where(me > 0, zrecv[me, :, at].astype(F32), 0.0)
        right = jnp.where(me < n - 1, zrecv[n, :, at].astype(F32), 0.0)
        gpad[pl.ds(EDGE, tokens), at] = (
            up_ref[:, at].astype(F32) + (total + left + right)
        ).astype(BF16)
        return 0

    lax.fori_loop(0, width // 128, sum_step, 0)

    def g_edge(d):
        to = (dp, jnp.clip(me + step_of[d], 0, n - 1))
        src = gpad.at[pl.ds(tokens if d == 0 else EDGE, EDGE)]
        dst = gpad.at[pl.ds(0 if d == 0 else EDGE + tokens, EDGE)]
        return send(src, dst, gs.at[d], gr.at[d], to)

    for d in ways:
        start(ahead[d] > 0, functools.partial(g_edge, d))
    ring_step(1, 1)

    def taps_step(i, _):
        at = pl.ds(pl.multiple_of(i * 128, 128), 128)
        g = gpad[pl.ds(EDGE, tokens), at].astype(F32)
        x = xpad[:, at].astype(F32)
        sums = [
            jnp.sum(g * x[EDGE - 3 + tap : EDGE - 3 + tap + tokens], axis=0, keepdims=True)
            for tap in range(KW)
        ]
        sums.append(jnp.zeros_like(sums[0]))
        k1[me, :, at] = jnp.concatenate(sums, axis=0)
        return 0

    lax.fori_loop(0, width // 128, taps_step, 0)

    def k1_send(j):
        to = lax.rem(me + j, n)
        return send(k1.at[me], k1.at[me], k1s.at[j], k1r.at[me], (dp, to))

    def k1_arrive(j):
        src = lax.rem(me + j, n)
        return send(k1.at[src], k1.at[src], k1s.at[j], k1r.at[src], (dp, src))

    for j in range(1, n):
        start(None, functools.partial(k1_send, j))
    for d in ways:

        @pl.when(room[d] > 0)
        def _(d=d):
            g_edge(d).wait_recv()

    def gin_step(i, _):
        at = pl.ds(pl.multiple_of(i * 128, 128), 128)
        g = gpad[:, at].astype(F32)
        taps = k_ref[:, at]
        total = g[EDGE : EDGE + tokens]
        for tap in range(KW):
            low = EDGE + 3 - tap
            total = total + taps[tap : tap + 1] * g[low : low + tokens]
        gin_ref[:, at] = total.astype(BF16)
        return 0

    lax.fori_loop(0, width // 128, gin_step, 0)
    ring_step(1, 2)
    for j in range(1, n):
        k1_arrive(j).wait_recv()
    taps_sum = k1[0]
    for j in range(1, n):
        taps_sum = taps_sum + k1[j]
    k2[dp, pl.ds(0, 8), :] = taps_sum
    k2[dp, pl.ds(8, 8), pl.ds(0, hidden)] = jnp.broadcast_to(bias[...], (8, hidden))
    if hidden < width:
        k2[dp, pl.ds(8, 8), pl.ds(hidden, width - hidden)] = jnp.zeros((8, width - hidden), F32)

    def k2_send(j):
        to = lax.rem(dp + j, dp_size)
        return send(k2.at[dp], k2.at[dp], k2s.at[j], k2r.at[dp], (to, me))

    def k2_arrive(j):
        src = lax.rem(dp + j, dp_size)
        return send(k2.at[src], k2.at[src], k2s.at[j], k2r.at[src], (src, me))

    for j in range(1, dp_size):
        start(None, functools.partial(k2_send, j))
    for s in range(3, last + 1):
        ring_step(1, s)
    for j in range(1, dp_size):
        k2_arrive(j).wait_recv()
    total = k2[0]
    for j in range(1, dp_size):
        total = total + k2[j]
    small_ref[...] = total
    ring_end(0)
    ring_end(1)
    for cond, make in pending:
        if cond is None:
            make().wait_send()
        else:

            @pl.when(cond)
            def _(make=make):
                make().wait_send()


def shards(n, dp_size, inputs, saved_hidden, upstream, w_in, w_out, kernel):
    chips = dp_size // 2
    tokens, width = inputs.shape[1:]
    hidden = w_in.shape[1]
    rows_in = width // (4 * chips)
    rows_out = -(-hidden // (4 * chips * 8)) * 8
    high = rows_out * 4 * chips
    dma = pltpu.SemaphoreType.DMA
    steps = 2 * (chips - 1)
    vmem = pl.BlockSpec(memory_space=pltpu.VMEM)
    shape = jax.ShapeDtypeStruct
    grad_inputs, grad_w_in, grad_w_out, small = pl.pallas_call(
        functools.partial(body, n, dp_size, rows_in, rows_out),
        out_shape=[
            shape((tokens, width), BF16),
            shape((2, 2, chips, rows_in, hidden), BF16),
            shape((2, 2, chips, rows_out, width), BF16),
            shape((16, width), F32),
        ],
        in_specs=[vmem] * 6,
        out_specs=[vmem] * 4,
        scratch_shapes=[
            pltpu.VMEM((n, tokens, high), BF16),
            pltpu.VMEM((n, tokens, hidden), BF16),
            pltpu.VMEM((n, tokens, width), BF16),
            pltpu.VMEM((n, tokens, width), BF16),
            pltpu.VMEM((n, tokens, width), BF16),
            pltpu.VMEM((n + 1, tokens, width), BF16),
            pltpu.VMEM((tokens + 2 * EDGE, width), BF16),
            pltpu.VMEM((tokens + 2 * EDGE, width), BF16),
            pltpu.VMEM((width, hidden), F32),
            pltpu.VMEM((high, width), F32),
            pltpu.VMEM((1, hidden), F32),
            pltpu.VMEM((2, chips, rows_in, hidden), BF16),
            pltpu.VMEM((2, chips, rows_out, width), BF16),
            pltpu.VMEM((2, chips, rows_in, hidden), BF16),
            pltpu.VMEM((2, chips, rows_out, width), BF16),
            pltpu.VMEM((2, chips - 1, rows_in, hidden), BF16),
            pltpu.VMEM((2, chips - 1, rows_out, width), BF16),
            pltpu.VMEM((2, chips - 1, rows_in, hidden), BF16),
            pltpu.VMEM((2, chips - 1, rows_out, width), BF16),
            pltpu.VMEM((n, 8, width), F32),
            pltpu.VMEM((dp_size, 16, width), F32),
            dma((2,)), dma((2,)),
            dma((2, n)), dma((2, n)),
            dma((2, n)), dma((2, n)),
            dma((2, n)), dma((2, n)),
            dma((2,)), dma((2,)),
            dma((2, 2, steps)), dma((2, 2, steps)),
            dma((2, 2, chips)), dma((2, 2, chips)),
            dma((2,)), dma((2,)),
            dma((n,)), dma((n,)),
            dma((dp_size,)), dma((dp_size,)),
        ],
        compiler_params=pltpu.CompilerParams(
            collective_id=0, has_side_effects=True, vmem_limit_bytes=67043328
        ),
    )(
        inputs[0],
        saved_hidden[0].reshape(n, tokens, hidden),
        upstream[0],
        w_in,
        w_out,
        kernel,
    )
    return (
        grad_inputs[None],
        grad_w_in.reshape(width, hidden).astype(F32),
        grad_w_out.reshape(high, width)[:hidden].astype(F32),
        small[8, :hidden],
        small[:KW],
    )


def solution(mesh):
    in_specs = (
        P("dp", "tp", None),
        P("dp", None, "tp"),
        P("dp", "tp", None),
        P(None, "tp"),
        P("tp", None),
        P(),
    )
    out_specs = (P("dp", "tp", None), P(None, "tp"), P("tp", None), P("tp"), P())
    return jax.shard_map(
        functools.partial(shards, mesh.shape["tp"], mesh.shape["dp"]),
        mesh=mesh,
        in_specs=in_specs,
        out_specs=out_specs,
        check_vma=False,
    )
```

```python
import functools

import jax
import jax.numpy as jnp
from jax import lax
from jax.experimental import pallas as pl
from jax.experimental.pallas import tpu as pltpu
from jax.sharding import PartitionSpec as P

KW = 7
EDGE = 16
F32 = jnp.float32
BF16 = jnp.bfloat16
MESH = pl.DeviceIdType.MESH


def dot(a, b, dims):
    return lax.dot_general(a, b, (dims, ((), ())), preferred_element_type=F32)


def chunk_of(size):
    return 256 if size % 256 == 0 else size


def body(
    n, dp_size, rows_in, rows_out, up_parts, mix_parts,
    x_hbm, h_hbm, up_hbm, win_hbm, wout_hbm, k_ref, gin_ref, small_ref, *refs,
):
    parts = up_parts + mix_parts
    finals, refs = refs[:parts], refs[parts:]
    accs, refs = refs[:parts], refs[parts:]
    psends, refs = refs[:parts], refs[parts:]
    precvs, refs = refs[:parts], refs[parts:]
    rsends, refs = refs[:parts], refs[parts:]
    rrecvs, refs = refs[:parts], refs[parts:]
    (
        h_ref, win_ref, wout_ref,
        act, gh, up_all, mix_all, part, zrecv, xpad, gpad, bias, k1, k2,
        ls, hl, ul, hs, hr, us, ur, zs, zr, ps, pr, rs, rr, ds, dr, gs, gr, k1s, k1r, k2s, k2r,
    ) = refs
    chips = dp_size // 2
    me = lax.axis_index("tp")
    dp = lax.axis_index("dp")
    core = lax.rem(dp, 2)
    chip = dp // 2
    tokens, width = x_hbm.shape
    hidden = h_ref.shape[2]
    up_wide = width // up_parts
    mix_wide = width // mix_parts
    tall = chunk_of(hidden)

    def flip(i):
        return jnp.where(i < chips // 2, i, chips // 2 + chips - 1 - i)

    pos = flip(chip)
    spots = (pos, lax.rem(chips - pos, chips))
    after = (
        flip(lax.rem(pos + 1, chips)) * 2 + core,
        flip(lax.rem(pos + chips - 1, chips)) * 2 + core,
    )
    partner = dp + 1 - 2 * core

    barrier = pltpu.get_barrier_semaphore()
    for j in range(1, n):
        pl.semaphore_signal(
            barrier, inc=1, device_id=(dp, lax.rem(me + j, n)), device_id_type=MESH
        )
    for j in range(1, dp_size):
        pl.semaphore_signal(
            barrier, inc=1, device_id=(lax.rem(dp + j, dp_size), me), device_id_type=MESH
        )
    pl.semaphore_wait(barrier, n - 1 + dp_size - 1)

    def send(src, dst, s, r, to):
        return pltpu.make_async_remote_copy(
            src_ref=src, dst_ref=dst, send_sem=s, recv_sem=r, device_id=to, device_id_type=MESH
        )

    pending = []

    def start(cond, make):
        if cond is None:
            make().start()
        else:

            @pl.when(cond)
            def _():
                make().start()

        pending.append((cond, make))

    ways = (0, 1)
    step_of = (1, -1)
    room = (me, n - 1 - me)
    ahead = (n - 1 - me, me)

    loads = [
        pltpu.make_async_copy(x_hbm, xpad.at[pl.ds(EDGE, tokens)], ls.at[0]),
        pltpu.make_async_copy(wout_hbm, wout_ref, ls.at[1]),
        pltpu.make_async_copy(win_hbm, win_ref, ls.at[2]),
    ]

    def load_hidden(j):
        b = lax.rem(me + j, n)
        return pltpu.make_async_copy(h_hbm.at[b], h_ref.at[b], hl.at[b])

    def load_up(c):
        src = up_hbm.at[:, pl.ds(c * up_wide, up_wide)]
        return pltpu.make_async_copy(src, up_all.at[c, me], ul.at[c])

    def place(k, b):
        return up_all.at[k, b] if k < up_parts else mix_all.at[k - up_parts, b]

    def chain(k, d, back):
        b = jnp.clip(me - step_of[d] * back, 0, n - 1)
        to = (dp, jnp.clip(me + step_of[d], 0, n - 1))
        src = place(k, b)
        if back == 0 and k < up_parts:
            src = up_hbm.at[:, pl.ds(k * up_wide, up_wide)]
        return send(src, place(k, b), us.at[k, d, b], ur.at[k, d, b], to)

    def x_edge(d):
        to = (dp, jnp.clip(me + step_of[d], 0, n - 1))
        src = x_hbm.at[pl.ds(tokens - EDGE if d == 0 else 0, EDGE)]
        dst = xpad.at[pl.ds(0 if d == 0 else EDGE + tokens, EDGE)]
        return send(src, dst, hs.at[d], hr.at[d], to)

    for d in ways:
        start(ahead[d] > 0, functools.partial(chain, 0, d, 0))
    for d in ways:
        start(ahead[d] > 0, functools.partial(x_edge, d))
    load_hidden(0).start()
    for c in range(up_parts):
        load_up(c).start()
    for load in loads:
        load.start()
    for j in range(1, n):
        load_hidden(j).start()

    if act.shape[2] > hidden:
        act[...] = jnp.zeros_like(act)
    bias[...] = jnp.zeros_like(bias)

    @pl.when(me == 0)
    def _():
        xpad[pl.ds(0, EDGE), :] = jnp.zeros((EDGE, width), BF16)
        gpad[pl.ds(0, EDGE), :] = jnp.zeros((EDGE, width), BF16)

    @pl.when(me == n - 1)
    def _():
        xpad[pl.ds(EDGE + tokens, EDGE), :] = jnp.zeros((EDGE, width), BF16)
        gpad[pl.ds(EDGE + tokens, EDGE), :] = jnp.zeros((EDGE, width), BF16)

    def gelu(b):
        pltpu.make_async_copy(h_hbm.at[b], h_ref.at[b], hl.at[b]).wait()

        def gelu_step(i, _):
            at = pl.ds(pl.multiple_of(i * 32, 32), 32)
            v = h_ref[b, at, :].astype(F32)
            cdf = 0.5 + 0.5 * lax.erf(v * 0.7071067811865476)
            act[b, at, pl.ds(0, hidden)] = (v * cdf).astype(BF16)
            gh[b, at, :] = (cdf + v * (0.3989422804014327 * jnp.exp(-0.5 * v * v))).astype(BF16)
            return 0

        lax.fori_loop(0, tokens // 32, gelu_step, 0)

    def mix():
        def mix_step(i, _):
            at = pl.ds(pl.multiple_of(i * 128, 128), 128)
            x = xpad[:, at].astype(F32)
            taps = k_ref[:, at]
            total = x[EDGE : EDGE + tokens]
            for tap in range(KW):
                low = EDGE - 3 + tap
                total = total + taps[tap : tap + 1] * x[low : low + tokens]
            c = i // (mix_wide // 128)
            lane = pl.ds(pl.multiple_of(lax.rem(i, mix_wide // 128) * 128, 128), 128)
            mix_all[c, me, :, lane] = total.astype(BF16)
            return 0

        lax.fori_loop(0, width // 128, mix_step, 0)

    def add_to(acc, at, value, first):
        if first:
            acc[at] = value
        else:
            acc[at] += value

    def out_dot(c, b, first):
        def out_step(i, _):
            at = pl.ds(pl.multiple_of(i * 128, 128), 128)
            value = dot(act[b], up_all[c, b, :, at], ((0,), (0,)))
            add_to(accs[c], (slice(None), at), value, first)
            return 0

        lax.fori_loop(0, up_wide // 128, out_step, 0)

    def back_dot(b):
        def back_step(i, _):
            at = pl.ds(pl.multiple_of(i * tall, tall), tall) if tall < hidden else pl.ds(0, hidden)
            back = None
            for c in range(up_parts):
                cols = pl.ds(c * up_wide, up_wide)
                term = dot(up_all[c, b], wout_ref[at, cols], ((1,), (1,)))
                back = term if back is None else back + term
            grad = (gh[b, :, at].astype(F32) * back).astype(BF16)
            gh[b, :, at] = grad
            bias[:, at] += jnp.sum(grad.astype(F32), axis=0, keepdims=True)
            return 0

        lax.fori_loop(0, hidden // tall, back_step, 0)

        wide = chunk_of(width)

        def part_step(i, _):
            at = pl.ds(pl.multiple_of(i * wide, wide), wide)
            part[b, :, at] = dot(gh[b], win_ref[at, :], ((1,), (1,))).astype(BF16)
            return 0

        lax.fori_loop(0, width // wide, part_step, 0)

    def in_dot(c, b, first):
        def in_step(i, _):
            at = pl.ds(pl.multiple_of(i * 128, 128), 128)
            value = dot(mix_all[c, b, :, at], gh[b], ((0,), (0,)))
            add_to(accs[up_parts + c], (at, slice(None)), value, first)
            return 0

        lax.fori_loop(0, mix_wide // 128, in_step, 0)

    def use(k, b, first=False):
        if k < up_parts:
            if k == 0:
                gelu(b)
            out_dot(k, b, first)
            if k == up_parts - 1:
                back_dot(b)
        else:
            in_dot(k - up_parts, b, first)

    sets = [
        (accs[w], psends[w], precvs[w], rsends[w], rrecvs[w], finals[w], rows_out if w < up_parts else rows_in)
        for w in range(parts)
    ]

    def rows_at(w, half, d, block):
        rows = sets[w][6]
        return pl.ds(pl.multiple_of(((half * 2 + d) * chips + block) * rows, 8), rows)

    def pair_copy(w):
        return send(sets[w][1], sets[w][2], ps.at[w], pr.at[w], (partner, me))

    def pair_start(w):
        for d in ways:
            for block in range(chips):
                sets[w][1][d, block] = sets[w][0][rows_at(w, 1 - core, d, block), :].astype(BF16)
        start(None, functools.partial(pair_copy, w))

    def own(w, d, block):
        return sets[w][0][rows_at(w, core, d, block), :] + sets[w][2][d, block].astype(F32)

    def ring_reduce(w, d, s):
        return send(
            sets[w][3].at[d, s], sets[w][4].at[d, s], rs.at[w, d, s], rr.at[w, d, s], (after[d], me)
        )

    def ring_gather(w, d, s):
        block = lax.rem(spots[d] + 1 - s + chips, chips)
        ref = sets[w][5].at[core, d, block]
        at = chips - 1 + s
        return send(ref, ref, rs.at[w, d, at], rr.at[w, d, at], (after[d], me))

    def across(w, d, block, half):
        ref = sets[w][5].at[half, d, block]
        return send(ref, ref, ds.at[w, d, block], dr.at[w, d, block], (partner, me))

    last = 2 * (chips - 1)

    def ring_step(w, s):
        if s > last:
            return
        if s == 0:
            pair_copy(w).wait_recv()
        for d in ways:
            spot = spots[d]
            if s < chips:
                block = lax.rem(spot - s + chips, chips)
                value = own(w, d, block)
                if s > 0:
                    ring_reduce(w, d, s - 1).wait_recv()
                    value = value + sets[w][4][d, s - 1].astype(F32)
                if s < chips - 1:
                    sets[w][3][d, s] = value.astype(BF16)
                    start(None, functools.partial(ring_reduce, w, d, s))
                    continue
                sets[w][5][core, d, block] = value.astype(BF16)
            else:
                block = lax.rem(spot + 1 - (s - chips + 1) + chips, chips)
                ring_arrive(w, d, s - chips).wait_recv()
            if s < last:
                start(None, functools.partial(ring_gather, w, d, s - chips + 1))
            start(None, functools.partial(across, w, d, block, core))

    def ring_arrive(w, d, s):
        block = lax.rem(spots[d] - s + chips, chips)
        ref = sets[w][5].at[core, d, block]
        at = chips - 1 + s
        return send(ref, ref, rs.at[w, d, at], rr.at[w, d, at], (after[d], me))

    def ring_end(w):
        for d in ways:
            for block in range(chips):
                across(w, d, block, 1 - core).wait_recv()

    def target(d, t, behind):
        place = room[d] - behind
        block = n - 1 - t + place
        return block if d == 0 else n - 1 - block

    def z_slot(d, block, owner):
        return jnp.where((block == owner) & (d == 1), n, block)

    def z_send(d, t):
        block = jnp.clip(target(d, t, 0), 0, n - 1)
        to = jnp.clip(me + step_of[d], 0, n - 1)
        return send(
            part.at[block], zrecv.at[z_slot(d, block, to)], zs.at[d, t], zr.at[d, t], (dp, to)
        )

    def z_arrive(d, t):
        block = jnp.clip(target(d, t, 1), 0, n - 1)
        slot = zrecv.at[z_slot(d, block, me)]
        return send(slot, slot, zs.at[d, t], zr.at[d, t], (dp, jnp.clip(me + 1, 0, n - 1)))

    def z_step(t):
        if t > n - 1:
            return
        for d in ways:
            if t > 0:

                @pl.when((room[d] >= 1) & (room[d] - 1 <= t - 1))
                def _(d=d):
                    z_arrive(d, t - 1).wait_recv()
                    if t < n - 1:
                        block = jnp.clip(target(d, t - 1, 1), 0, n - 1)
                        part[block] = (
                            part[block].astype(F32) + zrecv[z_slot(d, block, me)].astype(F32)
                        ).astype(BF16)

            if t < n - 1:
                start((room[d] <= t) & (ahead[d] > 0), functools.partial(z_send, d, t))

    active = []

    def tick():
        for item in list(active):
            ring_step(item[0], item[1])
            item[1] += 1
            if item[1] > last:
                active.remove(item)

    for k in range(parts):
        follow = k + 1
        if follow < parts and follow != up_parts:
            for d in ways:
                start((ahead[d] > 0) & (room[d] == 0), functools.partial(chain, follow, d, 0))
        if k == 0:
            load_up(0).wait()
        use_own = functools.partial(use, k, me, True)
        if k == up_parts - 1:
            if k > 0:
                load_up(k).wait()
            loads[1].wait()
            loads[2].wait()
        use_own()
        if k == 0:
            loads[0].wait()
            for d in ways:

                @pl.when(room[d] > 0)
                def _(d=d):
                    x_edge(d).wait_recv()

            mix()
        if follow == up_parts:
            for d in ways:
                start((ahead[d] > 0) & (room[d] == 0), functools.partial(chain, follow, d, 0))
        for back in range(1, n):
            for d in ways:

                @pl.when(room[d] >= back)
                def _(d=d):
                    chain(k, d, back).wait_recv()

                start((room[d] >= back) & (ahead[d] > 0), functools.partial(chain, k, d, back))
                if follow < parts:
                    start((room[d] == back) & (ahead[d] > 0), functools.partial(chain, follow, d, 0))
            for d in ways:

                @pl.when(room[d] >= back)
                def _(d=d):
                    use(k, jnp.clip(me - step_of[d] * back, 0, n - 1))

            tick()
        pair_start(k)
        active.append([k, 0])
        if k >= up_parts - 1:
            z_step(k - up_parts + 1)
    for t in range(mix_parts + 1, n - 1):
        z_step(t)
        tick()
    tick()
    tick()
    tick()
    z_step(n - 1)

    def own_up(i):
        c = i // (up_wide // 128)
        lane = pl.ds(pl.multiple_of(lax.rem(i, up_wide // 128) * 128, 128), 128)
        return up_all[c, me, :, lane].astype(F32)

    def sum_step(i, _):
        at = pl.ds(pl.multiple_of(i * 128, 128), 128)
        total = part[me, :, at].astype(F32)
        left = jnp.where(me > 0, zrecv[me, :, at].astype(F32), 0.0)
        right = jnp.where(me < n - 1, zrecv[n, :, at].astype(F32), 0.0)
        gpad[pl.ds(EDGE, tokens), at] = (
            own_up(i) + (total + left + right)
        ).astype(BF16)
        return 0

    lax.fori_loop(0, width // 128, sum_step, 0)

    def g_edge(d):
        to = (dp, jnp.clip(me + step_of[d], 0, n - 1))
        src = gpad.at[pl.ds(tokens if d == 0 else EDGE, EDGE)]
        dst = gpad.at[pl.ds(0 if d == 0 else EDGE + tokens, EDGE)]
        return send(src, dst, gs.at[d], gr.at[d], to)

    for d in ways:
        start(ahead[d] > 0, functools.partial(g_edge, d))
    tick()

    def taps_step(i, _):
        at = pl.ds(pl.multiple_of(i * 128, 128), 128)
        g = gpad[pl.ds(EDGE, tokens), at].astype(F32)
        x = xpad[:, at].astype(F32)
        sums = [
            jnp.sum(g * x[EDGE - 3 + tap : EDGE - 3 + tap + tokens], axis=0, keepdims=True)
            for tap in range(KW)
        ]
        sums.append(jnp.zeros_like(sums[0]))
        k1[me, :, at] = jnp.concatenate(sums, axis=0)
        return 0

    lax.fori_loop(0, width // 128, taps_step, 0)

    def k1_send(j):
        to = lax.rem(me + j, n)
        return send(k1.at[me], k1.at[me], k1s.at[j], k1r.at[me], (dp, to))

    def k1_arrive(j):
        src = lax.rem(me + j, n)
        return send(k1.at[src], k1.at[src], k1s.at[j], k1r.at[src], (dp, src))

    for j in range(1, n):
        start(None, functools.partial(k1_send, j))
    for d in ways:

        @pl.when(room[d] > 0)
        def _(d=d):
            g_edge(d).wait_recv()

    def gin_step(i, _):
        at = pl.ds(pl.multiple_of(i * 128, 128), 128)
        g = gpad[:, at].astype(F32)
        taps = k_ref[:, at]
        total = g[EDGE : EDGE + tokens]
        for tap in range(KW):
            low = EDGE + 3 - tap
            total = total + taps[tap : tap + 1] * g[low : low + tokens]
        gin_ref[:, at] = total.astype(BF16)
        return 0

    lax.fori_loop(0, width // 128, gin_step, 0)
    tick()
    for j in range(1, n):
        k1_arrive(j).wait_recv()
    taps_sum = k1[0]
    for j in range(1, n):
        taps_sum = taps_sum + k1[j]
    k2[dp, pl.ds(0, 8), :] = taps_sum
    k2[dp, pl.ds(8, 8), pl.ds(0, hidden)] = jnp.broadcast_to(bias[...], (8, hidden))
    if hidden < width:
        k2[dp, pl.ds(8, 8), pl.ds(hidden, width - hidden)] = jnp.zeros((8, width - hidden), F32)

    def k2_send(j):
        to = lax.rem(dp + j, dp_size)
        return send(k2.at[dp], k2.at[dp], k2s.at[j], k2r.at[dp], (to, me))

    def k2_arrive(j):
        src = lax.rem(dp + j, dp_size)
        return send(k2.at[src], k2.at[src], k2s.at[j], k2r.at[src], (src, me))

    for j in range(1, dp_size):
        start(None, functools.partial(k2_send, j))
    while active:
        tick()
    for j in range(1, dp_size):
        k2_arrive(j).wait_recv()
    total = k2[0]
    for j in range(1, dp_size):
        total = total + k2[j]
    small_ref[...] = total
    for w in range(parts):
        ring_end(w)
    for cond, make in pending:
        if cond is None:
            make().wait_send()
        else:

            @pl.when(cond)
            def _(make=make):
                make().wait_send()


def shards(n, dp_size, inputs, saved_hidden, upstream, w_in, w_out, kernel):
    chips = dp_size // 2
    tokens, width = inputs.shape[1:]
    hidden = w_in.shape[1]
    up_parts = 2 if width % 256 == 0 else 1
    mix_parts = 2 if width % (8 * chips * 8) == 0 and width % 256 == 0 else 1
    parts = up_parts + mix_parts
    rows_in = width // (4 * chips * mix_parts)
    rows_out = -(-hidden // (4 * chips * 8)) * 8
    high = rows_out * 4 * chips
    dma = pltpu.SemaphoreType.DMA
    steps = 2 * (chips - 1)
    vmem = pl.BlockSpec(memory_space=pltpu.VMEM)
    hbm = pl.BlockSpec(memory_space=pl.ANY)
    shape = jax.ShapeDtypeStruct
    sizes = [(rows_out, width // up_parts)] * up_parts + [(rows_in, hidden)] * mix_parts
    grad_inputs, small, *finals = pl.pallas_call(
        functools.partial(body, n, dp_size, rows_in, rows_out, up_parts, mix_parts),
        out_shape=[shape((tokens, width), BF16), shape((16, width), F32)]
        + [shape((2, 2, chips) + size, BF16) for size in sizes],
        in_specs=[hbm] * 5 + [vmem],
        out_specs=[vmem] * (2 + parts),
        scratch_shapes=[pltpu.VMEM((4 * chips * r, c), F32) for r, c in sizes]
        + [pltpu.VMEM((2, chips) + size, BF16) for size in sizes] * 2
        + [pltpu.VMEM((2, chips - 1) + size, BF16) for size in sizes] * 2
        + [
            pltpu.VMEM((n, tokens, hidden), BF16),
            pltpu.VMEM((width, hidden), BF16),
            pltpu.VMEM((hidden, width), BF16),
            pltpu.VMEM((n, tokens, high), BF16),
            pltpu.VMEM((n, tokens, hidden), BF16),
            pltpu.VMEM((up_parts, n, tokens, width // up_parts), BF16),
            pltpu.VMEM((mix_parts, n, tokens, width // mix_parts), BF16),
            pltpu.VMEM((n, tokens, width), BF16),
            pltpu.VMEM((n + 1, tokens, width), BF16),
            pltpu.VMEM((tokens + 2 * EDGE, width), BF16),
            pltpu.VMEM((tokens + 2 * EDGE, width), BF16),
            pltpu.VMEM((1, hidden), F32),
            pltpu.VMEM((n, 8, width), F32),
            pltpu.VMEM((dp_size, 16, width), F32),
            dma((3,)), dma((n,)), dma((up_parts,)),
            dma((2,)), dma((2,)),
            dma((parts, 2, n)), dma((parts, 2, n)),
            dma((2, n)), dma((2, n)),
            dma((parts,)), dma((parts,)),
            dma((parts, 2, steps)), dma((parts, 2, steps)),
            dma((parts, 2, chips)), dma((parts, 2, chips)),
            dma((2,)), dma((2,)),
            dma((n,)), dma((n,)),
            dma((dp_size,)), dma((dp_size,)),
        ],
        compiler_params=pltpu.CompilerParams(
            collective_id=0, has_side_effects=True, vmem_limit_bytes=67043328
        ),
    )(
        inputs[0],
        saved_hidden[0].reshape(n, tokens, hidden),
        upstream[0],
        w_in,
        w_out,
        kernel,
    )
    columns = [f.reshape(high, width // up_parts)[:hidden] for f in finals[:up_parts]]
    rows = [f.reshape(width // mix_parts, hidden) for f in finals[up_parts:]]
    return (
        grad_inputs[None],
        jnp.concatenate(rows, axis=0).astype(F32),
        jnp.concatenate(columns, axis=1).astype(F32),
        small[8, :hidden],
        small[:KW],
    )


def solution(mesh):
    in_specs = (
        P("dp", "tp", None),
        P("dp", None, "tp"),
        P("dp", "tp", None),
        P(None, "tp"),
        P("tp", None),
        P(),
    )
    out_specs = (P("dp", "tp", None), P(None, "tp"), P("tp", None), P("tp"), P())
    return jax.shard_map(
        functools.partial(shards, mesh.shape["tp"], mesh.shape["dp"]),
        mesh=mesh,
        in_specs=in_specs,
        out_specs=out_specs,
        check_vma=False,
    )
```

```python
import functools

import jax
import jax.numpy as jnp
from jax import lax
from jax.experimental import pallas as pl
from jax.experimental.pallas import tpu as pltpu
from jax.sharding import PartitionSpec as P

KW = 7
EDGE = 16
F32 = jnp.float32
BF16 = jnp.bfloat16
MESH = pl.DeviceIdType.MESH


def dot(a, b, dims):
    return lax.dot_general(a, b, (dims, ((), ())), preferred_element_type=F32)


def chunk_of(size):
    return 256 if size % 256 == 0 else size


def body(
    n, dp_size, rows_in, rows_out, up_parts, mix_parts,
    x_hbm, h_hbm, up_hbm, win_hbm, wout_hbm, k_ref, gin_ref, gk_ref, gb_ref, *refs,
):
    parts = up_parts + mix_parts
    finals, refs = refs[:parts], refs[parts:]
    accs, refs = refs[:parts], refs[parts:]
    psends, refs = refs[:parts], refs[parts:]
    precvs, refs = refs[:parts], refs[parts:]
    rsends, refs = refs[:parts], refs[parts:]
    rrecvs, refs = refs[:parts], refs[parts:]
    (
        h_ref, win_ref, wout_ref,
        act, gh, up_all, mix_all, part, zrecv, xpad, gpad, bias, k1, k2,
        ls, hl, ul, hs, hr, us, ur, zs, zr, ps, pr, rs, rr, ds, dr, gs, gr, k1s, k1r, k2s, k2r,
    ) = refs
    chips = dp_size // 2
    me = lax.axis_index("tp")
    dp = lax.axis_index("dp")
    core = lax.rem(dp, 2)
    chip = dp // 2
    tokens, width = x_hbm.shape
    hidden = h_ref.shape[2]
    up_wide = width // up_parts
    mix_wide = width // mix_parts
    tall = chunk_of(hidden)

    bits = chips.bit_length() - 1

    def mirror(i):
        return sum((i // 2**p) % 2 * 2 ** (bits - 1 - p) for p in range(bits))

    spots = (chip, mirror(chip))
    halves = [chips >> (s + 1) for s in range(bits)]
    starts = [sum(halves[:s]) for s in range(bits)]

    def span(d, s, other):
        h = halves[s]
        side = lax.rem(spots[d] // h, 2)
        low = spots[d] // h * h
        return low + (h - 2 * h * side if other else 0)

    def peer(d, s):
        h = halves[s]
        spot = spots[d] + h - 2 * h * lax.rem(spots[d] // h, 2)
        return (mirror(spot) if d else spot) * 2 + core

    partner = dp + 1 - 2 * core

    barrier = pltpu.get_barrier_semaphore()
    for j in range(1, n):
        pl.semaphore_signal(
            barrier, inc=1, device_id=(dp, lax.rem(me + j, n)), device_id_type=MESH
        )
    for j in range(1, dp_size):
        pl.semaphore_signal(
            barrier, inc=1, device_id=(lax.rem(dp + j, dp_size), me), device_id_type=MESH
        )
    pl.semaphore_wait(barrier, n - 1 + dp_size - 1)

    def send(src, dst, s, r, to):
        return pltpu.make_async_remote_copy(
            src_ref=src, dst_ref=dst, send_sem=s, recv_sem=r, device_id=to, device_id_type=MESH
        )

    pending = []

    def start(cond, make):
        if cond is None:
            make().start()
        else:

            @pl.when(cond)
            def _():
                make().start()

        pending.append((cond, make))

    ways = (0, 1)
    step_of = (1, -1)
    room = (me, n - 1 - me)
    ahead = (n - 1 - me, me)

    loads = [
        pltpu.make_async_copy(x_hbm, xpad.at[pl.ds(EDGE, tokens)], ls.at[0]),
        pltpu.make_async_copy(wout_hbm, wout_ref, ls.at[1]),
        pltpu.make_async_copy(win_hbm, win_ref, ls.at[2]),
    ]

    def load_hidden(j):
        b = lax.rem(me + j, n)
        return pltpu.make_async_copy(h_hbm.at[b], h_ref.at[b], hl.at[b])

    def load_up(c):
        src = up_hbm.at[:, pl.ds(c * up_wide, up_wide)]
        return pltpu.make_async_copy(src, up_all.at[c, me], ul.at[c])

    def place(k, b):
        return up_all.at[k, b] if k < up_parts else mix_all.at[k - up_parts, b]

    def chain(k, d, back):
        b = jnp.clip(me - step_of[d] * back, 0, n - 1)
        to = (dp, jnp.clip(me + step_of[d], 0, n - 1))
        src = place(k, b)
        if back == 0 and k < up_parts:
            src = up_hbm.at[:, pl.ds(k * up_wide, up_wide)]
        return send(src, place(k, b), us.at[k, d, b], ur.at[k, d, b], to)

    def x_edge(d):
        to = (dp, jnp.clip(me + step_of[d], 0, n - 1))
        src = x_hbm.at[pl.ds(tokens - EDGE if d == 0 else 0, EDGE)]
        dst = xpad.at[pl.ds(0 if d == 0 else EDGE + tokens, EDGE)]
        return send(src, dst, hs.at[d], hr.at[d], to)

    for k in range(2):
        for d in ways:
            start(ahead[d] > 0, functools.partial(chain, k, d, 0))
    for d in ways:
        start(ahead[d] > 0, functools.partial(x_edge, d))
    load_hidden(0).start()
    for c in range(up_parts):
        load_up(c).start()
    for load in loads:
        load.start()
    for j in range(1, n):
        load_hidden(j).start()

    if act.shape[2] > hidden:
        act[...] = jnp.zeros_like(act)
    bias[...] = jnp.zeros_like(bias)

    @pl.when(me == 0)
    def _():
        xpad[pl.ds(0, EDGE), :] = jnp.zeros((EDGE, width), BF16)
        gpad[pl.ds(0, EDGE), :] = jnp.zeros((EDGE, width), BF16)

    @pl.when(me == n - 1)
    def _():
        xpad[pl.ds(EDGE + tokens, EDGE), :] = jnp.zeros((EDGE, width), BF16)
        gpad[pl.ds(EDGE + tokens, EDGE), :] = jnp.zeros((EDGE, width), BF16)

    def gelu(b):
        pltpu.make_async_copy(h_hbm.at[b], h_ref.at[b], hl.at[b]).wait()

        def gelu_step(i, _):
            at = pl.ds(pl.multiple_of(i * 32, 32), 32)
            v = h_ref[b, at, :].astype(F32)
            cdf = 0.5 + 0.5 * lax.erf(v * 0.7071067811865476)
            act[b, at, pl.ds(0, hidden)] = (v * cdf).astype(BF16)
            gh[b, at, :] = (cdf + v * (0.3989422804014327 * jnp.exp(-0.5 * v * v))).astype(BF16)
            return 0

        lax.fori_loop(0, tokens // 32, gelu_step, 0)

    def mix():
        def mix_step(i, _):
            at = pl.ds(pl.multiple_of(i * 128, 128), 128)
            x = xpad[:, at].astype(F32)
            taps = k_ref[:, at]
            total = x[EDGE : EDGE + tokens]
            for tap in range(KW):
                low = EDGE - 3 + tap
                total = total + taps[tap : tap + 1] * x[low : low + tokens]
            c = i // (mix_wide // 128)
            lane = pl.ds(pl.multiple_of(lax.rem(i, mix_wide // 128) * 128, 128), 128)
            mix_all[c, me, :, lane] = total.astype(BF16)
            return 0

        lax.fori_loop(0, width // 128, mix_step, 0)

    def add_to(acc, at, value, first):
        if first:
            acc[at] = value
        else:
            acc[at] += value

    def out_dot(c, b, first):
        def out_step(i, _):
            at = pl.ds(pl.multiple_of(i * 128, 128), 128)
            value = dot(act[b], up_all[c, b, :, at], ((0,), (0,)))
            add_to(accs[c], (slice(None), at), value, first)
            return 0

        lax.fori_loop(0, up_wide // 128, out_step, 0)

    def back_dot(b):
        def back_step(i, _):
            at = pl.ds(pl.multiple_of(i * tall, tall), tall) if tall < hidden else pl.ds(0, hidden)
            back = None
            for c in range(up_parts):
                cols = pl.ds(c * up_wide, up_wide)
                term = dot(up_all[c, b], wout_ref[at, cols], ((1,), (1,)))
                back = term if back is None else back + term
            grad = (gh[b, :, at].astype(F32) * back).astype(BF16)
            gh[b, :, at] = grad
            bias[:, at] += jnp.sum(grad.astype(F32), axis=0, keepdims=True)
            return 0

        lax.fori_loop(0, hidden // tall, back_step, 0)

        wide = chunk_of(width)

        def part_step(i, _):
            at = pl.ds(pl.multiple_of(i * wide, wide), wide)
            part[b, :, at] = dot(gh[b], win_ref[at, :], ((1,), (1,))).astype(BF16)
            return 0

        lax.fori_loop(0, width // wide, part_step, 0)

    def in_dot(c, b, first):
        def in_step(i, _):
            at = pl.ds(pl.multiple_of(i * 128, 128), 128)
            value = dot(mix_all[c, b, :, at], gh[b], ((0,), (0,)))
            add_to(accs[up_parts + c], (at, slice(None)), value, first)
            return 0

        lax.fori_loop(0, mix_wide // 128, in_step, 0)

    def use(k, b, first=False):
        if k < up_parts:
            if k == 0:
                gelu(b)
            out_dot(k, b, first)
            if k == up_parts - 1:
                back_dot(b)
        else:
            in_dot(k - up_parts, b, first)

    sets = [
        (accs[w], psends[w], precvs[w], rsends[w], rrecvs[w], finals[w], rows_out if w < up_parts else rows_in)
        for w in range(parts)
    ]

    def rows_at(w, half, d, block):
        rows = sets[w][6]
        return pl.ds(pl.multiple_of(((half * 2 + d) * chips + block) * rows, 8), rows)

    def pair_copy(w):
        return send(sets[w][1], sets[w][2], ps.at[w], pr.at[w], (partner, me))

    def pair_start(w):
        for d in ways:
            for block in range(chips):
                sets[w][1][d, block] = sets[w][0][rows_at(w, 1 - core, d, block), :].astype(BF16)
        start(None, functools.partial(pair_copy, w))

    def own(w, d, block):
        return sets[w][0][rows_at(w, core, d, block), :] + sets[w][2][d, block].astype(F32)

    def ring_reduce(w, d, s):
        at = pl.ds(starts[s], halves[s])
        return send(
            sets[w][3].at[d, at], sets[w][4].at[d, at], rs.at[w, d, s], rr.at[w, d, s],
            (peer(d, s), me),
        )

    def ring_gather(w, d, s, other):
        ref = sets[w][5].at[core, d, pl.ds(span(d, s, other), halves[s])]
        at = 2 * bits - 1 - s
        return send(ref, ref, rs.at[w, d, at], rr.at[w, d, at], (peer(d, s), me))

    def across(w, d, s, half):
        if s == bits:
            ref = sets[w][5].at[half, d, pl.ds(spots[d], 1)]
        else:
            ref = sets[w][5].at[half, d, pl.ds(span(d, s, True), halves[s])]
        return send(ref, ref, ds.at[w, d, s], dr.at[w, d, s], (partner, me))

    last = 2 * bits

    def ring_step(w, s):
        acc, _, _, rsend, rrecv, final, _ = sets[w]
        if s == 0:
            pair_copy(w).wait_recv()
        for d in ways:
            if s <= bits:
                if s > 0:
                    ring_reduce(w, d, s - 1).wait_recv()

                def value(block, s=s, d=d):
                    if s == 0:
                        return own(w, d, block)
                    got = rrecv[d, starts[s - 1] + block - span(d, s - 1, False)].astype(F32)
                    if s == 1:
                        return own(w, d, block) + got
                    return acc[rows_at(w, core, d, block), :] + got

                if s == bits:
                    final[core, d, spots[d]] = value(spots[d]).astype(BF16)
                    start(None, functools.partial(ring_gather, w, d, s - 1, False))
                    start(None, functools.partial(across, w, d, bits, core))
                    continue
                for j in range(halves[s]):
                    rsend[d, starts[s] + j] = value(span(d, s, True) + j).astype(BF16)
                start(None, functools.partial(ring_reduce, w, d, s))
                if s > 0:
                    for j in range(halves[s]):
                        block = span(d, s, False) + j
                        acc[rows_at(w, core, d, block), :] = value(block)
            else:
                step = 2 * bits - s
                ring_gather(w, d, step, True).wait_recv()
                if step > 0:
                    start(None, functools.partial(ring_gather, w, d, step - 1, False))
                start(None, functools.partial(across, w, d, step, core))

    def ring_end(w):
        for d in ways:
            for s in range(bits + 1):
                across(w, d, s, 1 - core).wait_recv()

    def target(d, t, behind):
        place = room[d] - behind
        block = n - 1 - t + place
        return block if d == 0 else n - 1 - block

    def z_slot(d, block, owner):
        return jnp.where((block == owner) & (d == 1), n, block)

    def z_send(d, t):
        block = jnp.clip(target(d, t, 0), 0, n - 1)
        to = jnp.clip(me + step_of[d], 0, n - 1)
        return send(
            part.at[block], zrecv.at[z_slot(d, block, to)], zs.at[d, t], zr.at[d, t], (dp, to)
        )

    def z_arrive(d, t):
        block = jnp.clip(target(d, t, 1), 0, n - 1)
        slot = zrecv.at[z_slot(d, block, me)]
        return send(slot, slot, zs.at[d, t], zr.at[d, t], (dp, jnp.clip(me + 1, 0, n - 1)))

    def z_step(t):
        if t > n - 1:
            return
        for d in ways:
            if t > 0:

                @pl.when((room[d] >= 1) & (room[d] - 1 <= t - 1))
                def _(d=d):
                    z_arrive(d, t - 1).wait_recv()
                    if t < n - 1:
                        block = jnp.clip(target(d, t - 1, 1), 0, n - 1)
                        part[block] = (
                            part[block].astype(F32) + zrecv[z_slot(d, block, me)].astype(F32)
                        ).astype(BF16)

            if t < n - 1:
                start((room[d] <= t) & (ahead[d] > 0), functools.partial(z_send, d, t))

    active = []

    def tick():
        for item in list(active):
            ring_step(item[0], item[1])
            item[1] += 1
            if item[1] > last:
                active.remove(item)

    for k in range(parts):
        follow = k + 2
        if k == 0:
            load_up(0).wait()
        use_own = functools.partial(use, k, me, True)
        if k == up_parts - 1:
            if k > 0:
                load_up(k).wait()
            loads[1].wait()
            loads[2].wait()
        use_own()
        if k == 0:
            loads[0].wait()
            for d in ways:

                @pl.when(room[d] > 0)
                def _(d=d):
                    x_edge(d).wait_recv()

            mix()
        if follow < parts:
            for d in ways:
                start((ahead[d] > 0) & (room[d] == 0), functools.partial(chain, follow, d, 0))
        for back in range(1, n):
            for d in ways:

                @pl.when(room[d] >= back)
                def _(d=d):
                    chain(k, d, back).wait_recv()

                start((room[d] >= back) & (ahead[d] > 0), functools.partial(chain, k, d, back))
                if follow < parts:
                    start((room[d] == back) & (ahead[d] > 0), functools.partial(chain, follow, d, 0))
            for d in ways:

                @pl.when(room[d] >= back)
                def _(d=d):
                    use(k, jnp.clip(me - step_of[d] * back, 0, n - 1))

            tick()
        pair_start(k)
        active.append([k, 0])
        if k >= up_parts - 1:
            z_step(k - up_parts + 1)
    for t in range(mix_parts + 1, n - 1):
        z_step(t)
        tick()
    tick()
    tick()
    tick()
    z_step(n - 1)

    def own_up(i):
        c = i // (up_wide // 128)
        lane = pl.ds(pl.multiple_of(lax.rem(i, up_wide // 128) * 128, 128), 128)
        return up_all[c, me, :, lane].astype(F32)

    def sum_step(i, _):
        at = pl.ds(pl.multiple_of(i * 128, 128), 128)
        total = part[me, :, at].astype(F32)
        left = jnp.where(me > 0, zrecv[me, :, at].astype(F32), 0.0)
        right = jnp.where(me < n - 1, zrecv[n, :, at].astype(F32), 0.0)
        gpad[pl.ds(EDGE, tokens), at] = (
            own_up(i) + (total + left + right)
        ).astype(BF16)
        return 0

    lax.fori_loop(0, width // 128, sum_step, 0)

    def g_edge(d):
        to = (dp, jnp.clip(me + step_of[d], 0, n - 1))
        src = gpad.at[pl.ds(tokens if d == 0 else EDGE, EDGE)]
        dst = gpad.at[pl.ds(0 if d == 0 else EDGE + tokens, EDGE)]
        return send(src, dst, gs.at[d], gr.at[d], to)

    for d in ways:
        start(ahead[d] > 0, functools.partial(g_edge, d))
    tick()

    def taps_step(i, _):
        at = pl.ds(pl.multiple_of(i * 128, 128), 128)
        g = gpad[pl.ds(EDGE, tokens), at].astype(F32)
        x = xpad[:, at].astype(F32)
        sums = [
            jnp.sum(g * x[EDGE - 3 + tap : EDGE - 3 + tap + tokens], axis=0, keepdims=True)
            for tap in range(KW)
        ]
        sums.append(jnp.zeros_like(sums[0]))
        k1[me, :, at] = jnp.concatenate(sums, axis=0)
        return 0

    lax.fori_loop(0, width // 128, taps_step, 0)

    def k1_send(j):
        to = lax.rem(me + j, n)
        return send(k1.at[me], k1.at[me], k1s.at[j], k1r.at[me], (dp, to))

    def k1_arrive(j):
        src = lax.rem(me + j, n)
        return send(k1.at[src], k1.at[src], k1s.at[j], k1r.at[src], (dp, src))

    for j in range(1, n):
        start(None, functools.partial(k1_send, j))
    for d in ways:

        @pl.when(room[d] > 0)
        def _(d=d):
            g_edge(d).wait_recv()

    def gin_step(i, _):
        at = pl.ds(pl.multiple_of(i * 128, 128), 128)
        g = gpad[:, at].astype(F32)
        taps = k_ref[:, at]
        total = g[EDGE : EDGE + tokens]
        for tap in range(KW):
            low = EDGE + 3 - tap
            total = total + taps[tap : tap + 1] * g[low : low + tokens]
        gin_ref[:, at] = total.astype(BF16)
        return 0

    lax.fori_loop(0, width // 128, gin_step, 0)
    tick()
    for j in range(1, n):
        k1_arrive(j).wait_recv()
    taps_sum = k1[0]
    for j in range(1, n):
        taps_sum = taps_sum + k1[j]
    k2[dp, pl.ds(0, 8), :] = taps_sum
    k2[dp, pl.ds(8, 8), pl.ds(0, hidden)] = jnp.broadcast_to(bias[...], (8, hidden))
    if hidden < width:
        k2[dp, pl.ds(8, 8), pl.ds(hidden, width - hidden)] = jnp.zeros((8, width - hidden), F32)

    def k2_send(j):
        to = lax.rem(dp + j, dp_size)
        return send(k2.at[dp], k2.at[dp], k2s.at[j], k2r.at[dp], (to, me))

    def k2_arrive(j):
        src = lax.rem(dp + j, dp_size)
        return send(k2.at[src], k2.at[src], k2s.at[j], k2r.at[src], (src, me))

    for j in range(1, dp_size):
        start(None, functools.partial(k2_send, j))
    while active:
        tick()
    for j in range(1, dp_size):
        k2_arrive(j).wait_recv()
    total = k2[0]
    for j in range(1, dp_size):
        total = total + k2[j]
    gk_ref[...] = total[:KW]
    gb_ref[...] = total[8:9, :hidden]
    for w in range(parts):
        ring_end(w)
    for cond, make in pending:
        if cond is None:
            make().wait_send()
        else:

            @pl.when(cond)
            def _(make=make):
                make().wait_send()


def shards(n, dp_size, inputs, saved_hidden, upstream, w_in, w_out, kernel):
    chips = dp_size // 2
    tokens, width = inputs.shape[1:]
    hidden = w_in.shape[1]
    up_parts = 2
    mix_parts = 2 if width % (8 * chips * 8) == 0 and width % 256 == 0 else 1
    parts = up_parts + mix_parts
    rows_in = width // (4 * chips * mix_parts)
    rows_out = -(-hidden // (4 * chips * 8)) * 8
    high = rows_out * 4 * chips
    dma = pltpu.SemaphoreType.DMA
    bits = chips.bit_length() - 1
    vmem = pl.BlockSpec(memory_space=pltpu.VMEM)
    hbm = pl.BlockSpec(memory_space=pl.ANY)
    shape = jax.ShapeDtypeStruct
    sizes = [(rows_out, width // up_parts)] * up_parts + [(rows_in, hidden)] * mix_parts
    grad_inputs, grad_kernel, grad_bias, *finals = pl.pallas_call(
        functools.partial(body, n, dp_size, rows_in, rows_out, up_parts, mix_parts),
        out_shape=[shape((tokens, width), BF16), shape((KW, width), F32), shape((1, hidden), F32)]
        + [shape((2, 2, chips) + size, BF16) for size in sizes],
        in_specs=[hbm] * 5 + [vmem],
        out_specs=[vmem] * (3 + parts),
        scratch_shapes=[pltpu.VMEM((4 * chips * r, c), F32) for r, c in sizes]
        + [pltpu.VMEM((2, chips) + size, BF16) for size in sizes] * 2
        + [pltpu.VMEM((2, chips - 1) + size, BF16) for size in sizes] * 2
        + [
            pltpu.VMEM((n, tokens, hidden), BF16),
            pltpu.VMEM((width, hidden), BF16),
            pltpu.VMEM((hidden, width), BF16),
            pltpu.VMEM((n, tokens, high), BF16),
            pltpu.VMEM((n, tokens, hidden), BF16),
            pltpu.VMEM((up_parts, n, tokens, width // up_parts), BF16),
            pltpu.VMEM((mix_parts, n, tokens, width // mix_parts), BF16),
            pltpu.VMEM((n, tokens, width), BF16),
            pltpu.VMEM((n + 1, tokens, width), BF16),
            pltpu.VMEM((tokens + 2 * EDGE, width), BF16),
            pltpu.VMEM((tokens + 2 * EDGE, width), BF16),
            pltpu.VMEM((1, hidden), F32),
            pltpu.VMEM((n, 8, width), F32),
            pltpu.VMEM((dp_size, 16, width), F32),
            dma((3,)), dma((n,)), dma((up_parts,)),
            dma((2,)), dma((2,)),
            dma((parts, 2, n)), dma((parts, 2, n)),
            dma((2, n)), dma((2, n)),
            dma((parts,)), dma((parts,)),
            dma((parts, 2, 2 * bits)), dma((parts, 2, 2 * bits)),
            dma((parts, 2, bits + 1)), dma((parts, 2, bits + 1)),
            dma((2,)), dma((2,)),
            dma((n,)), dma((n,)),
            dma((dp_size,)), dma((dp_size,)),
        ],
        compiler_params=pltpu.CompilerParams(
            collective_id=0, has_side_effects=True, vmem_limit_bytes=67043328
        ),
    )(
        inputs[0],
        saved_hidden[0].reshape(n, tokens, hidden),
        upstream[0],
        w_in,
        w_out,
        kernel,
    )
    columns = [f.reshape(high, width // up_parts)[:hidden] for f in finals[:up_parts]]
    rows = [f.reshape(width // mix_parts, hidden) for f in finals[up_parts:]]
    return (
        grad_inputs[None],
        jnp.concatenate(rows, axis=0).astype(F32),
        jnp.concatenate(columns, axis=1).astype(F32),
        grad_bias[0],
        grad_kernel,
    )


def solution(mesh):
    in_specs = (
        P("dp", "tp", None),
        P("dp", None, "tp"),
        P("dp", "tp", None),
        P(None, "tp"),
        P("tp", None),
        P(),
    )
    out_specs = (P("dp", "tp", None), P(None, "tp"), P("tp", None), P("tp"), P())
    return jax.shard_map(
        functools.partial(shards, mesh.shape["tp"], mesh.shape["dp"]),
        mesh=mesh,
        in_specs=in_specs,
        out_specs=out_specs,
        check_vma=False,
    )
```

```python
import functools

import jax
import jax.numpy as jnp
from jax import lax
from jax.experimental import pallas as pl
from jax.experimental.pallas import tpu as pltpu
from jax.sharding import PartitionSpec as P

KW = 7
EDGE = 16
F32 = jnp.float32
BF16 = jnp.bfloat16
MESH = pl.DeviceIdType.MESH


def dot(a, b, dims):
    return lax.dot_general(a, b, (dims, ((), ())), preferred_element_type=F32)


def chunk_of(size):
    return 256 if size % 256 == 0 else size


def body(
    n, dp_size, rows_in, rows_out, up_parts, mix_parts,
    x_hbm, h_hbm, up_hbm, win_hbm, wout_hbm, k_ref, gin_ref, gk_ref, gb_ref, *refs,
):
    parts = up_parts + mix_parts
    finals, refs = refs[:parts], refs[parts:]
    accs, refs = refs[:parts], refs[parts:]
    psends, refs = refs[:parts], refs[parts:]
    precvs, refs = refs[:parts], refs[parts:]
    rsends, refs = refs[:parts], refs[parts:]
    rrecvs, refs = refs[:parts], refs[parts:]
    (
        h_ref, win_ref, wout_ref,
        act, gh, up_all, mix_all, part, zrecv, xpad, gpad, bias, k1, k2,
        ls, hl, ul, hs, hr, us, ur, zs, zr, ps, pr, rs, rr, ds, dr, gs, gr, k1s, k1r, k2s, k2r,
    ) = refs
    chips = dp_size // 2
    me = lax.axis_index("tp")
    dp = lax.axis_index("dp")
    core = lax.rem(dp, 2)
    chip = dp // 2
    tokens, width = x_hbm.shape
    hidden = h_ref.shape[2]
    up_wide = width // up_parts
    mix_wide = width // mix_parts
    tall = chunk_of(hidden)

    bits = chips.bit_length() - 1

    def mirror(i):
        return sum((i // 2**p) % 2 * 2 ** (bits - 1 - p) for p in range(bits))

    spots = (chip, mirror(chip))
    halves = [chips >> (s + 1) for s in range(bits)]
    starts = [sum(halves[:s]) for s in range(bits)]

    def span(d, s, other):
        h = halves[s]
        side = lax.rem(spots[d] // h, 2)
        low = spots[d] // h * h
        return low + (h - 2 * h * side if other else 0)

    def peer(d, s):
        h = halves[s]
        spot = spots[d] + h - 2 * h * lax.rem(spots[d] // h, 2)
        return (mirror(spot) if d else spot) * 2 + core

    partner = dp + 1 - 2 * core

    barrier = pltpu.get_barrier_semaphore()
    for j in range(1, n):
        pl.semaphore_signal(
            barrier, inc=1, device_id=(dp, lax.rem(me + j, n)), device_id_type=MESH
        )
    for j in range(1, dp_size):
        pl.semaphore_signal(
            barrier, inc=1, device_id=(lax.rem(dp + j, dp_size), me), device_id_type=MESH
        )
    pl.semaphore_wait(barrier, n - 1 + dp_size - 1)

    def send(src, dst, s, r, to):
        return pltpu.make_async_remote_copy(
            src_ref=src, dst_ref=dst, send_sem=s, recv_sem=r, device_id=to, device_id_type=MESH
        )

    pending = []

    def start(cond, make):
        if cond is None:
            make().start()
        else:

            @pl.when(cond)
            def _():
                make().start()

        pending.append((cond, make))

    ways = (0, 1)
    step_of = (1, -1)
    room = (me, n - 1 - me)
    ahead = (n - 1 - me, me)

    loads = [
        pltpu.make_async_copy(x_hbm, xpad.at[pl.ds(EDGE, tokens)], ls.at[0]),
        pltpu.make_async_copy(wout_hbm, wout_ref, ls.at[1]),
        pltpu.make_async_copy(win_hbm, win_ref, ls.at[2]),
    ]

    def load_hidden(j):
        b = lax.rem(me + j, n)
        return pltpu.make_async_copy(h_hbm.at[b], h_ref.at[b], hl.at[b])

    def load_up(c):
        src = up_hbm.at[:, pl.ds(c * up_wide, up_wide)]
        return pltpu.make_async_copy(src, up_all.at[c, me], ul.at[c])

    def place(k, b):
        return up_all.at[k, b] if k < up_parts else mix_all.at[k - up_parts, b]

    def chain(k, d, back):
        b = jnp.clip(me - step_of[d] * back, 0, n - 1)
        to = (dp, jnp.clip(me + step_of[d], 0, n - 1))
        src = place(k, b)
        if back == 0 and k < up_parts:
            src = up_hbm.at[:, pl.ds(k * up_wide, up_wide)]
        return send(src, place(k, b), us.at[k, d, b], ur.at[k, d, b], to)

    def x_edge(d):
        to = (dp, jnp.clip(me + step_of[d], 0, n - 1))
        src = x_hbm.at[pl.ds(tokens - EDGE if d == 0 else 0, EDGE)]
        dst = xpad.at[pl.ds(0 if d == 0 else EDGE + tokens, EDGE)]
        return send(src, dst, hs.at[d], hr.at[d], to)

    for d in ways:
        start(ahead[d] > 0, functools.partial(chain, 0, d, 0))
    for d in ways:
        start(ahead[d] > 0, functools.partial(x_edge, d))
    load_hidden(0).start()
    for c in range(up_parts):
        load_up(c).start()
    for load in loads:
        load.start()
    for j in range(1, n):
        load_hidden(j).start()

    if act.shape[2] > hidden:
        act[...] = jnp.zeros_like(act)
    bias[...] = jnp.zeros_like(bias)

    @pl.when(me == 0)
    def _():
        xpad[pl.ds(0, EDGE), :] = jnp.zeros((EDGE, width), BF16)
        gpad[pl.ds(0, EDGE), :] = jnp.zeros((EDGE, width), BF16)

    @pl.when(me == n - 1)
    def _():
        xpad[pl.ds(EDGE + tokens, EDGE), :] = jnp.zeros((EDGE, width), BF16)
        gpad[pl.ds(EDGE + tokens, EDGE), :] = jnp.zeros((EDGE, width), BF16)

    def gelu(b):
        pltpu.make_async_copy(h_hbm.at[b], h_ref.at[b], hl.at[b]).wait()

        def gelu_step(i, _):
            at = pl.ds(pl.multiple_of(i * 32, 32), 32)
            v = h_ref[b, at, :].astype(F32)
            cdf = 0.5 + 0.5 * lax.erf(v * 0.7071067811865476)
            act[b, at, pl.ds(0, hidden)] = (v * cdf).astype(BF16)
            gh[b, at, :] = (cdf + v * (0.3989422804014327 * jnp.exp(-0.5 * v * v))).astype(BF16)
            return 0

        lax.fori_loop(0, tokens // 32, gelu_step, 0)

    def mix():
        def mix_step(i, _):
            at = pl.ds(pl.multiple_of(i * 128, 128), 128)
            x = xpad[:, at].astype(F32)
            taps = k_ref[:, at]
            total = x[EDGE : EDGE + tokens]
            for tap in range(KW):
                low = EDGE - 3 + tap
                total = total + taps[tap : tap + 1] * x[low : low + tokens]
            c = i // (mix_wide // 128)
            lane = pl.ds(pl.multiple_of(lax.rem(i, mix_wide // 128) * 128, 128), 128)
            mix_all[c, me, :, lane] = total.astype(BF16)
            return 0

        lax.fori_loop(0, width // 128, mix_step, 0)

    def add_to(acc, at, value, first):
        if first:
            acc[at] = value
        else:
            acc[at] += value

    def out_dot(c, b, first):
        high = chunk_of(act.shape[2])

        def out_step(i, _):
            at = pl.ds(pl.multiple_of(i * high, high), high)
            value = dot(act[b, :, at], up_all[c, b], ((0,), (0,)))
            add_to(accs[c], (at, slice(None)), value, first)
            return 0

        lax.fori_loop(0, act.shape[2] // high, out_step, 0)

    def back_dot(b):
        def back_step(i, _):
            at = pl.ds(pl.multiple_of(i * tall, tall), tall) if tall < hidden else pl.ds(0, hidden)
            back = None
            for c in range(up_parts):
                cols = pl.ds(c * up_wide, up_wide)
                term = dot(up_all[c, b], wout_ref[at, cols], ((1,), (1,)))
                back = term if back is None else back + term
            grad = (gh[b, :, at].astype(F32) * back).astype(BF16)
            gh[b, :, at] = grad
            bias[:, at] += jnp.sum(grad.astype(F32), axis=0, keepdims=True)
            return 0

        lax.fori_loop(0, hidden // tall, back_step, 0)

        wide = chunk_of(width)

        def part_step(i, _):
            at = pl.ds(pl.multiple_of(i * wide, wide), wide)
            part[b, :, at] = dot(gh[b], win_ref[at, :], ((1,), (1,))).astype(BF16)
            return 0

        lax.fori_loop(0, width // wide, part_step, 0)

    def in_dot(c, b, first):
        def in_step(i, _):
            at = pl.ds(pl.multiple_of(i * 128, 128), 128)
            value = dot(mix_all[c, b, :, at], gh[b], ((0,), (0,)))
            add_to(accs[up_parts + c], (at, slice(None)), value, first)
            return 0

        lax.fori_loop(0, mix_wide // 128, in_step, 0)

    def use(k, b, first=False):
        if k < up_parts:
            if k == 0:
                gelu(b)
            out_dot(k, b, first)
            if k == up_parts - 1:
                back_dot(b)
        else:
            in_dot(k - up_parts, b, first)

    sets = [
        (accs[w], psends[w], precvs[w], rsends[w], rrecvs[w], finals[w], rows_out if w < up_parts else rows_in)
        for w in range(parts)
    ]

    def rows_at(w, half, d, block):
        rows = sets[w][6]
        return pl.ds(pl.multiple_of(((half * 2 + d) * chips + block) * rows, 8), rows)

    def pair_copy(w):
        return send(sets[w][1], sets[w][2], ps.at[w], pr.at[w], (partner, me))

    def pair_start(w):
        for d in ways:
            for block in range(chips):
                sets[w][1][d, block] = sets[w][0][rows_at(w, 1 - core, d, block), :].astype(BF16)
        start(None, functools.partial(pair_copy, w))

    def own(w, d, block):
        return sets[w][0][rows_at(w, core, d, block), :] + sets[w][2][d, block].astype(F32)

    def ring_reduce(w, d, s):
        at = pl.ds(starts[s], halves[s])
        return send(
            sets[w][3].at[d, at], sets[w][4].at[d, at], rs.at[w, d, s], rr.at[w, d, s],
            (peer(d, s), me),
        )

    def ring_gather(w, d, s, other):
        ref = sets[w][5].at[core, d, pl.ds(span(d, s, other), halves[s])]
        at = 2 * bits - 1 - s
        return send(ref, ref, rs.at[w, d, at], rr.at[w, d, at], (peer(d, s), me))

    def across(w, d, s, half):
        if s == bits:
            ref = sets[w][5].at[half, d, pl.ds(spots[d], 1)]
        else:
            ref = sets[w][5].at[half, d, pl.ds(span(d, s, True), halves[s])]
        return send(ref, ref, ds.at[w, d, s], dr.at[w, d, s], (partner, me))

    last = 2 * bits

    def ring_step(w, s):
        acc, _, _, rsend, rrecv, final, _ = sets[w]
        if s == 0:
            pair_copy(w).wait_recv()
        for d in ways:
            if s <= bits:
                if s > 0:
                    ring_reduce(w, d, s - 1).wait_recv()

                def value(block, s=s, d=d):
                    if s == 0:
                        return own(w, d, block)
                    got = rrecv[d, starts[s - 1] + block - span(d, s - 1, False)].astype(F32)
                    if s == 1:
                        return own(w, d, block) + got
                    return acc[rows_at(w, core, d, block), :] + got

                if s == bits:
                    final[core, d, spots[d]] = value(spots[d]).astype(BF16)
                    start(None, functools.partial(ring_gather, w, d, s - 1, False))
                    start(None, functools.partial(across, w, d, bits, core))
                    continue
                for j in range(halves[s]):
                    rsend[d, starts[s] + j] = value(span(d, s, True) + j).astype(BF16)
                start(None, functools.partial(ring_reduce, w, d, s))
                if s > 0:
                    for j in range(halves[s]):
                        block = span(d, s, False) + j
                        acc[rows_at(w, core, d, block), :] = value(block)
            else:
                step = 2 * bits - s
                ring_gather(w, d, step, True).wait_recv()
                if step > 0:
                    start(None, functools.partial(ring_gather, w, d, step - 1, False))
                start(None, functools.partial(across, w, d, step, core))

    def ring_end(w):
        for d in ways:
            for s in range(bits + 1):
                across(w, d, s, 1 - core).wait_recv()

    def target(d, t, behind):
        place = room[d] - behind
        block = n - 1 - t + place
        return block if d == 0 else n - 1 - block

    def z_slot(d, block, owner):
        return jnp.where((block == owner) & (d == 1), n, block)

    def z_send(d, t):
        block = jnp.clip(target(d, t, 0), 0, n - 1)
        to = jnp.clip(me + step_of[d], 0, n - 1)
        return send(
            part.at[block], zrecv.at[z_slot(d, block, to)], zs.at[d, t], zr.at[d, t], (dp, to)
        )

    def z_arrive(d, t):
        block = jnp.clip(target(d, t, 1), 0, n - 1)
        slot = zrecv.at[z_slot(d, block, me)]
        return send(slot, slot, zs.at[d, t], zr.at[d, t], (dp, jnp.clip(me + 1, 0, n - 1)))

    def z_step(t):
        if t > n - 1:
            return
        for d in ways:
            if t > 0:

                @pl.when((room[d] >= 1) & (room[d] - 1 <= t - 1))
                def _(d=d):
                    z_arrive(d, t - 1).wait_recv()
                    if t < n - 1:
                        block = jnp.clip(target(d, t - 1, 1), 0, n - 1)
                        part[block] = (
                            part[block].astype(F32) + zrecv[z_slot(d, block, me)].astype(F32)
                        ).astype(BF16)

            if t < n - 1:
                start((room[d] <= t) & (ahead[d] > 0), functools.partial(z_send, d, t))

    active = []

    def tick():
        for item in list(active):
            ring_step(item[0], item[1])
            item[1] += 1
            if item[1] > last:
                active.remove(item)

    for k in range(parts):
        follow = k + 1
        if k == 0:
            load_up(0).wait()
        use_own = functools.partial(use, k, me, True)
        if k == up_parts - 1:
            if k > 0:
                load_up(k).wait()
            loads[1].wait()
            loads[2].wait()
        use_own()
        if k == 0:
            loads[0].wait()
            for d in ways:

                @pl.when(room[d] > 0)
                def _(d=d):
                    x_edge(d).wait_recv()

            mix()
        if follow < parts:
            for d in ways:
                start((ahead[d] > 0) & (room[d] == 0), functools.partial(chain, follow, d, 0))
        for back in range(1, n):
            for d in ways:

                @pl.when(room[d] >= back)
                def _(d=d):
                    chain(k, d, back).wait_recv()

                start((room[d] >= back) & (ahead[d] > 0), functools.partial(chain, k, d, back))
                if follow < parts:
                    start((room[d] == back) & (ahead[d] > 0), functools.partial(chain, follow, d, 0))
            for d in ways:

                @pl.when(room[d] >= back)
                def _(d=d):
                    use(k, jnp.clip(me - step_of[d] * back, 0, n - 1))

            tick()
        pair_start(k)
        active.append([k, 0])
        if k >= up_parts - 1:
            z_step(k - up_parts + 1)
    for t in range(mix_parts + 1, n - 1):
        z_step(t)
        tick()
    tick()
    tick()
    tick()
    z_step(n - 1)

    def own_up(i):
        c = i // (up_wide // 128)
        lane = pl.ds(pl.multiple_of(lax.rem(i, up_wide // 128) * 128, 128), 128)
        return up_all[c, me, :, lane].astype(F32)

    def sum_step(i, _):
        at = pl.ds(pl.multiple_of(i * 128, 128), 128)
        total = part[me, :, at].astype(F32)
        left = jnp.where(me > 0, zrecv[me, :, at].astype(F32), 0.0)
        right = jnp.where(me < n - 1, zrecv[n, :, at].astype(F32), 0.0)
        gpad[pl.ds(EDGE, tokens), at] = (
            own_up(i) + (total + left + right)
        ).astype(BF16)
        return 0

    lax.fori_loop(0, width // 128, sum_step, 0)

    def g_edge(d):
        to = (dp, jnp.clip(me + step_of[d], 0, n - 1))
        src = gpad.at[pl.ds(tokens if d == 0 else EDGE, EDGE)]
        dst = gpad.at[pl.ds(0 if d == 0 else EDGE + tokens, EDGE)]
        return send(src, dst, gs.at[d], gr.at[d], to)

    for d in ways:
        start(ahead[d] > 0, functools.partial(g_edge, d))
    tick()

    def taps_step(i, _):
        at = pl.ds(pl.multiple_of(i * 128, 128), 128)
        g = gpad[pl.ds(EDGE, tokens), at].astype(F32)
        x = xpad[:, at].astype(F32)
        sums = [
            jnp.sum(g * x[EDGE - 3 + tap : EDGE - 3 + tap + tokens], axis=0, keepdims=True)
            for tap in range(KW)
        ]
        sums.append(jnp.zeros_like(sums[0]))
        k1[me, :, at] = jnp.concatenate(sums, axis=0)
        return 0

    lax.fori_loop(0, width // 128, taps_step, 0)

    def k1_send(j):
        to = lax.rem(me + j, n)
        return send(k1.at[me], k1.at[me], k1s.at[j], k1r.at[me], (dp, to))

    def k1_arrive(j):
        src = lax.rem(me + j, n)
        return send(k1.at[src], k1.at[src], k1s.at[j], k1r.at[src], (dp, src))

    for j in range(1, n):
        start(None, functools.partial(k1_send, j))
    for d in ways:

        @pl.when(room[d] > 0)
        def _(d=d):
            g_edge(d).wait_recv()

    def gin_step(i, _):
        at = pl.ds(pl.multiple_of(i * 128, 128), 128)
        g = gpad[:, at].astype(F32)
        taps = k_ref[:, at]
        total = g[EDGE : EDGE + tokens]
        for tap in range(KW):
            low = EDGE + 3 - tap
            total = total + taps[tap : tap + 1] * g[low : low + tokens]
        gin_ref[:, at] = total.astype(BF16)
        return 0

    lax.fori_loop(0, width // 128, gin_step, 0)
    tick()
    for j in range(1, n):
        k1_arrive(j).wait_recv()
    taps_sum = k1[0]
    for j in range(1, n):
        taps_sum = taps_sum + k1[j]
    k2[dp, pl.ds(0, 8), :] = taps_sum
    k2[dp, pl.ds(8, 8), pl.ds(0, hidden)] = jnp.broadcast_to(bias[...], (8, hidden))
    if hidden < width:
        k2[dp, pl.ds(8, 8), pl.ds(hidden, width - hidden)] = jnp.zeros((8, width - hidden), F32)

    def k2_send(j):
        to = lax.rem(dp + j, dp_size)
        return send(k2.at[dp], k2.at[dp], k2s.at[j], k2r.at[dp], (to, me))

    def k2_arrive(j):
        src = lax.rem(dp + j, dp_size)
        return send(k2.at[src], k2.at[src], k2s.at[j], k2r.at[src], (src, me))

    for j in range(1, dp_size):
        start(None, functools.partial(k2_send, j))
    while active:
        tick()
    for j in range(1, dp_size):
        k2_arrive(j).wait_recv()
    total = k2[0]
    for j in range(1, dp_size):
        total = total + k2[j]
    gk_ref[...] = total[:KW]
    gb_ref[...] = total[8:9, :hidden]
    for w in range(parts):
        ring_end(w)
    for cond, make in pending:
        if cond is None:
            make().wait_send()
        else:

            @pl.when(cond)
            def _(make=make):
                make().wait_send()


def shards(n, dp_size, inputs, saved_hidden, upstream, w_in, w_out, kernel):
    chips = dp_size // 2
    tokens, width = inputs.shape[1:]
    hidden = w_in.shape[1]
    up_parts = 2
    mix_parts = 2 if width % (8 * chips * 8) == 0 and width % 256 == 0 else 1
    parts = up_parts + mix_parts
    rows_in = width // (4 * chips * mix_parts)
    rows_out = -(-hidden // (4 * chips * 8)) * 8
    high = rows_out * 4 * chips
    dma = pltpu.SemaphoreType.DMA
    bits = chips.bit_length() - 1
    vmem = pl.BlockSpec(memory_space=pltpu.VMEM)
    hbm = pl.BlockSpec(memory_space=pl.ANY)
    shape = jax.ShapeDtypeStruct
    sizes = [(rows_out, width // up_parts)] * up_parts + [(rows_in, hidden)] * mix_parts
    grad_inputs, grad_kernel, grad_bias, *finals = pl.pallas_call(
        functools.partial(body, n, dp_size, rows_in, rows_out, up_parts, mix_parts),
        out_shape=[shape((tokens, width), BF16), shape((KW, width), F32), shape((1, hidden), F32)]
        + [shape((2, 2, chips) + size, BF16) for size in sizes],
        in_specs=[hbm] * 5 + [vmem],
        out_specs=[vmem] * (3 + parts),
        scratch_shapes=[pltpu.VMEM((4 * chips * r, c), F32) for r, c in sizes]
        + [pltpu.VMEM((2, chips) + size, BF16) for size in sizes] * 2
        + [pltpu.VMEM((2, chips - 1) + size, BF16) for size in sizes] * 2
        + [
            pltpu.VMEM((n, tokens, hidden), BF16),
            pltpu.VMEM((width, hidden), BF16),
            pltpu.VMEM((hidden, width), BF16),
            pltpu.VMEM((n, tokens, high), BF16),
            pltpu.VMEM((n, tokens, hidden), BF16),
            pltpu.VMEM((up_parts, n, tokens, width // up_parts), BF16),
            pltpu.VMEM((mix_parts, n, tokens, width // mix_parts), BF16),
            pltpu.VMEM((n, tokens, width), BF16),
            pltpu.VMEM((n + 1, tokens, width), BF16),
            pltpu.VMEM((tokens + 2 * EDGE, width), BF16),
            pltpu.VMEM((tokens + 2 * EDGE, width), BF16),
            pltpu.VMEM((1, hidden), F32),
            pltpu.VMEM((n, 8, width), F32),
            pltpu.VMEM((dp_size, 16, width), F32),
            dma((3,)), dma((n,)), dma((up_parts,)),
            dma((2,)), dma((2,)),
            dma((parts, 2, n)), dma((parts, 2, n)),
            dma((2, n)), dma((2, n)),
            dma((parts,)), dma((parts,)),
            dma((parts, 2, 2 * bits)), dma((parts, 2, 2 * bits)),
            dma((parts, 2, bits + 1)), dma((parts, 2, bits + 1)),
            dma((2,)), dma((2,)),
            dma((n,)), dma((n,)),
            dma((dp_size,)), dma((dp_size,)),
        ],
        compiler_params=pltpu.CompilerParams(
            collective_id=0, has_side_effects=True, vmem_limit_bytes=67043328
        ),
    )(
        inputs[0],
        saved_hidden[0].reshape(n, tokens, hidden),
        upstream[0],
        w_in,
        w_out,
        kernel,
    )
    columns = [f.reshape(high, width // up_parts)[:hidden] for f in finals[:up_parts]]
    rows = [f.reshape(width // mix_parts, hidden) for f in finals[up_parts:]]
    return (
        grad_inputs[None],
        jnp.concatenate(rows, axis=0).astype(F32),
        jnp.concatenate(columns, axis=1).astype(F32),
        grad_bias[0],
        grad_kernel,
    )


def solution(mesh):
    in_specs = (
        P("dp", "tp", None),
        P("dp", None, "tp"),
        P("dp", "tp", None),
        P(None, "tp"),
        P("tp", None),
        P(),
    )
    out_specs = (P("dp", "tp", None), P(None, "tp"), P("tp", None), P("tp"), P())
    return jax.shard_map(
        functools.partial(shards, mesh.shape["tp"], mesh.shape["dp"]),
        mesh=mesh,
        in_specs=in_specs,
        out_specs=out_specs,
        check_vma=False,
    )
```
